128 devices in a mesh: kz: 4 (over z), jy: 4 (over y), ix: 8 (over x, core).
Axes of the slice: x: 4, y: 4, z: 4, core: 2. Of those that a mesh axis runs over, the one named last changes fastest.
Arguments:
- tensor: float32 [1536, 128, 1536], P('ix', 'jy', 'kz')
- b_init: float32 [128, 64], P(('jy', 'ix', 'kz'))
- c_init: float32 [1536, 64], P(('kz', 'ix', 'jy'))
- ridge: float32 [], replicated
Outputs:
- output 1: float32 [1536, 64], P(('ix', 'jy', 'kz'))
- output 2: float32 [128, 64], P(('jy', 'ix', 'kz'))
- output 3: float32 [1536, 64], P(('kz', 'ix', 'jy'))
- output 4: float32 [64], replicated
All inputs are finite; a program needn't handle non-finite values.
Results may differ from the reference program's by a relative error of at most 0.001.
Values are sent between devices in bfloat16 or wider.
A program may use at most 1 GiB of HBM per device.

```python
import jax
import jax.numpy as jnp
from jax import lax

I_DEV = 192
J_DEV = 32
K_DEV = 384
RANK = 64
GRID_I = 8
GRID_J = 4
GRID_K = 4
SWEEPS = 2

DIM_I = I_DEV * GRID_I
DIM_J = J_DEV * GRID_J
DIM_K = K_DEV * GRID_K


def unit_columns(matrix):
    return matrix / jnp.sqrt(jnp.sum(matrix * matrix, axis=0, keepdims=True))


def collinear_factor(rng_key, row_count, common_share):
    key_base, key_common = jax.random.split(rng_key)
    base_draw = jax.random.normal(key_base, (row_count, RANK), jnp.float32)
    common = jax.random.normal(key_common, (row_count, 1), jnp.float32)
    return unit_columns((1.0 - common_share) ** 0.5 * base_draw + common_share ** 0.5 * common)


def planted_tensor(fac_a, fac_b, fac_c):
    def one_block(a_block):
        pair_rows = (a_block[:, None, :] * fac_b[None, :, :]).reshape(I_DEV * DIM_J, RANK)
        return jnp.dot(pair_rows, fac_c.T, preferred_element_type=jnp.float32).reshape(I_DEV, DIM_J, DIM_K)
    blocks = lax.map(one_block, fac_a.reshape(GRID_I, I_DEV, RANK))
    return blocks.reshape(DIM_I, DIM_J, DIM_K)


def setup_inputs(seed: int = 0) -> dict:
    keys = jax.random.split(jax.random.key(seed), 8)
    true_a = collinear_factor(keys[0], DIM_I, 0.5)
    true_b = collinear_factor(keys[1], DIM_J, 0.5)
    true_c = collinear_factor(keys[2], DIM_K, 0.5)
    col_weights = jax.random.uniform(keys[3], (RANK,), jnp.float32, 0.5, 1.5)
    clean = planted_tensor(true_a * col_weights[None, :], true_b, true_c)
    clean = clean / jnp.sqrt(jnp.mean(clean * clean))
    tensor = clean + 0.2 * jax.random.normal(keys[4], (DIM_I, DIM_J, DIM_K), jnp.float32)
    b_init = collinear_factor(keys[5], DIM_J, 0.7)
    c_init = collinear_factor(keys[6], DIM_K, 0.7)
    ridge = jax.random.uniform(keys[7], (), jnp.float32, 0.03, 0.1)
    return {'tensor': tensor, 'b_init': b_init, 'c_init': c_init, 'ridge': ridge}


def reference(tensor, b_init, c_init, ridge):
    x_blocks = tensor.reshape(GRID_I, I_DEV, DIM_J, DIM_K)
    eye_mat = jnp.eye(RANK, dtype=jnp.float32)

    def gram_of(factor):
        return jnp.dot(factor.T, factor, preferred_element_type=jnp.float32)

    def update(mttkrp, gram_one, gram_two):
        system = gram_one * gram_two + ridge * eye_mat
        raw_rows = jnp.linalg.solve(system, mttkrp.T).T
        col_norms = jnp.sqrt(jnp.sum(raw_rows * raw_rows, axis=0))
        return raw_rows / col_norms[None, :], col_norms

    def mttkrp_a(fac_b, fac_c):
        def per_block(x_block):
            partial_t = jnp.einsum('ijk,kr->ijr', x_block, fac_c)
            return jnp.einsum('ijr,jr->ir', partial_t, fac_b)
        return lax.map(per_block, x_blocks).reshape(DIM_I, RANK)

    def mttkrp_b(fac_a, fac_c):
        def scan_step(running, block_pair):
            x_block, a_block = block_pair
            partial_t = jnp.einsum('ijk,kr->ijr', x_block, fac_c)
            return running + jnp.einsum('ijr,ir->jr', partial_t, a_block), None
        total_sum, unused_tail = lax.scan(scan_step, jnp.zeros((DIM_J, RANK), jnp.float32), (x_blocks, fac_a.reshape(GRID_I, I_DEV, RANK)))
        return total_sum

    def mttkrp_c(fac_a, fac_b):
        def scan_step(running, block_pair):
            x_block, a_block = block_pair
            partial_t = jnp.einsum('ijk,jr->ikr', x_block, fac_b)
            return running + jnp.einsum('ikr,ir->kr', partial_t, a_block), None
        total_sum, unused_tail = lax.scan(scan_step, jnp.zeros((DIM_K, RANK), jnp.float32), (x_blocks, fac_a.reshape(GRID_I, I_DEV, RANK)))
        return total_sum

    fac_b = b_init
    fac_c = c_init
    fac_a = None
    col_norms = None
    for sweep_idx in range(SWEEPS):
        fac_a, col_norms = update(mttkrp_a(fac_b, fac_c), gram_of(fac_b), gram_of(fac_c))
        fac_b, col_norms = update(mttkrp_b(fac_a, fac_c), gram_of(fac_a), gram_of(fac_c))
        fac_c, col_norms = update(mttkrp_c(fac_a, fac_b), gram_of(fac_a), gram_of(fac_b))
    return fac_a, fac_b, fac_c, col_norms
```

```python
import functools

import jax
import jax.numpy as jnp
from jax import lax
from jax.experimental import pallas as pl
from jax.experimental.pallas import tpu as pltpu
from jax.sharding import PartitionSpec as P

MESH = pl.DeviceIdType.MESH
F32 = jnp.float32
BF16 = jnp.bfloat16
SWEEPS = 2
RANK = 64
LANES = 128
CHUNKS = 8
GRAM_ROWS = 40


def full_dot(left, right):
    return jnp.dot(left, right, precision=lax.Precision.HIGHEST, preferred_element_type=F32)


def full_dot_nt(left, right):
    return lax.dot_general(left, right, (((1,), (1,)), ((), ())), precision=lax.Precision.HIGHEST, preferred_element_type=F32)


def piece_dot(left, right):
    return jnp.dot(left, right, preferred_element_type=F32)


def split3(value):
    high = value.astype(BF16)
    rest = value - high.astype(F32)
    mid = rest.astype(BF16)
    low = (rest - mid.astype(F32)).astype(BF16)
    return high, mid, low


def iota(shape, dim):
    return lax.broadcasted_iota(jnp.int32, shape, dim)


def left_half(shape):
    return iota(shape, 1) < RANK


def swap_halves(value):
    return pltpu.roll(value, RANK, 1)


def pack_dup(dup):
    half = dup.shape[0] // 2
    return jnp.where(left_half((half, LANES)), dup[:half], dup[half:])


def unpack_dup(packed):
    swapped = swap_halves(packed)
    is_left = left_half(packed.shape)
    return jnp.concatenate([jnp.where(is_left, packed, swapped), jnp.where(is_left, swapped, packed)], axis=0)


def eye_mask():
    return iota((RANK, LANES), 0) == iota((RANK, LANES), 1)


def diag_row(gram):
    return jnp.sum(jnp.where(eye_mask(), gram, 0.0), axis=0, keepdims=True)


def diag_col(gram):
    return jnp.sum(jnp.where(eye_mask(), gram, 0.0), axis=1, keepdims=True)


def eliminate(state):
    rows = iota((RANK, LANES), 0)
    for t in range(8):
        col = jnp.broadcast_to(state[:, t:t + 1], (RANK, LANES))
        row = state[t:t + 1, :] / col[t:t + 1, :]
        state = jnp.where(rows == t, row, state - col * row)
    state = jnp.concatenate([state[8:], state[:8]], axis=0)
    return pltpu.roll(state, LANES - 8, 1)


class Links:
    def __init__(self, send_sem, recv_sem):
        self.send_sem, self.recv_sem = send_sem, recv_sem
        self.used = 0
        self.sent = []

    def copy(self, src, dst, device):
        n = self.used
        self.used += 1
        desc = pltpu.make_async_remote_copy(
            src_ref=src, dst_ref=dst, send_sem=self.send_sem.at[n], recv_sem=self.recv_sem.at[n],
            device_id=device, device_id_type=MESH)
        desc.start()
        self.sent.append(desc)
        return desc

    def drain(self):
        for desc in self.sent:
            desc.wait_send()


def count_copies(nx, ny, nz):
    x, y, z = nx - 1, ny - 1, nz - 1
    a = 2 * (y + z)
    b = 1 + 2 * (x + z)
    c = 2 + 2 * (x + y)
    return SWEEPS * a + (SWEEPS + 1) * (b + c) + (SWEEPS + 1) * (y + z) + SWEEPS * (1 + x) + 1 + x


def kernel(sizes, x_hbm, b_in, c_in, lam_ref, a_out, b_out, c_out, w_out,
           x_stage, x_hi, x_mid, x_low, t_ref, pa_ref, a_dup, a_pack, acc_ref, b_pad, c_pad, inv_ref,
           a_buf, b_core, b_buf, c_part, c_rs, c_buf, ct_ref, g_core, g_buf, s_core, s_buf,
           load_sem, send_sem, recv_sem):
    nx, ny, nz = sizes
    kz, jy, ix = lax.axis_index("kz"), lax.axis_index("jy"), lax.axis_index("ix")
    xx, core = lax.div(ix, 2), lax.rem(ix, 2)
    where = {"x": xx, "y": jy, "z": kz}
    count = {"x": nx, "y": ny, "z": nz}

    def peer(axis, d):
        if axis == "x":
            return {"ix": 2 * lax.rem(xx + d, nx) + core}
        if axis == "y":
            return {"jy": lax.rem(jy + d, ny)}
        return {"kz": lax.rem(kz + d, nz)}

    partner = {"ix": 2 * xx + (1 - core)}
    links = Links(send_sem, recv_sem)

    rows_x, width = x_stage.shape
    rows_i = rows_x // b_buf_rows(b_core)
    rows_j = 2 * b_core.shape[2]
    step = rows_x // CHUNKS

    loads = [
        pltpu.make_async_copy(x_hbm.at[pl.ds(n * step, step)], x_stage.at[pl.ds(n * step, step)], load_sem.at[n])
        for n in range(CHUNKS)
    ]
    for load in loads:
        load.start()

    barrier = pltpu.get_barrier_semaphore()
    others = [partner] + [peer(axis, d) for axis in "xyz" for d in range(1, count[axis])]
    for other in others:
        pl.semaphore_signal(barrier, inc=1, device_id=other, device_id_type=MESH)
    pl.semaphore_wait(barrier, len(others))

    def spread(slots, axis):
        mine = slots.at[where[axis]]
        return [links.copy(mine, mine, peer(axis, d)) for d in range(1, count[axis])]

    def gather(slots, axis, copies, op=jnp.add):
        for desc in copies:
            desc.wait_recv()
        total = slots[0]
        for n in range(1, count[axis]):
            total = op(total, slots[n])
        return total

    class PlaneSum:
        def __init__(self, buf, axes):
            self.buf = buf
            self.orders = (axes, axes[::-1])

        def start(self, halves):
            self.copies = []
            for h, half in enumerate(halves):
                first = self.orders[h][0]
                slots = self.buf.at[0, h]
                slots[where[first]] = half
                self.copies.append(spread(slots, first))

        def turn(self):
            copies, self.copies = self.copies, []
            for h in range(2):
                first, second = self.orders[h]
                total = gather(self.buf.at[0, h], first, copies[h])
                slots = self.buf.at[1, h]
                slots[where[second]] = total
                self.copies.append(spread(slots, second))

        def finish(self):
            return jnp.concatenate(
                [gather(self.buf.at[1, h], self.orders[h][1], self.copies[h]) for h in range(2)], axis=0)

    def halves_of(value):
        half = value.shape[0] // 2
        return value[:half], value[half:]

    class SumA(PlaneSum):
        def __init__(self, n):
            super().__init__(a_buf.at[n], "yz")

    class SumB(PlaneSum):
        def __init__(self, n):
            super().__init__(b_buf.at[n], "xz")
            self.pair = b_core.at[n]

        def begin(self, packed):
            self.pair[core] = packed
            self.pair_copy = links.copy(self.pair.at[core], self.pair.at[core], partner)

        def join(self):
            self.pair_copy.wait_recv()
            self.start(halves_of(self.pair[0] + self.pair[1]))

    class SumC(PlaneSum):
        def __init__(self, n):
            super().__init__(c_buf.at[n], "xy")
            self.part, self.got, self.ct = c_part.at[n], c_rs.at[n], ct_ref.at[n]

        def begin(self, part):
            self.part[...] = part
            self.pair_copy = links.copy(self.part.at[pl.ds(pl.multiple_of(32 * (1 - core), 32), 32)], self.got, partner)

        def join(self):
            self.pair_copy.wait_recv()
            self.start(halves_of(self.part[pl.ds(pl.multiple_of(32 * core, 32), 32), :] + self.got[...]))

        def share(self):
            mine = pl.ds(pl.multiple_of(32 * core, 32), 32)
            self.ct[mine, :] = self.finish()
            self.pair_copy = links.copy(self.ct.at[mine], self.ct.at[mine], partner)

        def result(self):
            self.pair_copy.wait_recv()
            return self.ct[...]

    class GramSum:
        def __init__(self, n, axis):
            self.slots, self.axis = g_buf.at[n], axis

        def start(self, packed, tile=None):
            mine = where[self.axis]
            self.slots[mine, 0:32] = packed
            self.slots[mine, 32:GRAM_ROWS] = jnp.zeros((8, LANES), F32) if tile is None else tile
            self.copies = spread(self.slots, self.axis)

        def finish(self):
            for desc in self.copies:
                desc.wait_recv()
            total, peak = self.slots[0, 0:32], self.slots[0, 32:GRAM_ROWS]
            for n in range(1, count[self.axis]):
                total = total + self.slots[n, 0:32]
                peak = jnp.maximum(peak, self.slots[n, 32:GRAM_ROWS])
            return unpack_dup(total), peak

    class GramSumA(GramSum):
        def __init__(self, n, m):
            super().__init__(n, "x")
            self.pair = g_core.at[m]

        def begin(self, packed):
            self.pair[core] = packed
            self.pair_copy = links.copy(self.pair.at[core], self.pair.at[core], partner)

        def join(self):
            self.pair_copy.wait_recv()
            self.start(self.pair[0] + self.pair[1])

    def gram_of_packed(packed):
        prod = full_dot(jnp.transpose(packed), packed)
        gram = prod[:RANK] + swap_halves(prod[RANK:])
        return jnp.where(left_half((32, LANES)), gram[:32], swap_halves(gram[32:]))

    def gram_of_ct(ct):
        gram = full_dot_nt(ct, jnp.concatenate([ct, ct], axis=0))
        return jnp.where(left_half((32, LANES)), gram[:32], gram[32:])

    nb, nc, na = b_in.shape[0], c_in.shape[0], a_out.shape[0]
    b_pad[...] = jnp.zeros_like(b_pad)
    c_pad[...] = jnp.zeros_like(c_pad)
    b_pad[0:nb, 0:RANK] = b_in[...]
    c_pad[0:nc, 0:RANK] = c_in[...]
    b_base = (ix * nz + kz) * nb
    c_base = (ix * ny + jy) * nc
    a_base = (jy * nz + kz) * na

    def chooser(base, used, size, pad):
        t = iota((pad, size), 0)
        return jnp.where((iota((pad, size), 1) == t + base) & (t < used), 1.0, 0.0).astype(F32)

    b_own = b_pad[...] + swap_halves(b_pad[...])
    b_rows = full_dot(jnp.transpose(chooser(b_base, nb, rows_j, b_pad.shape[0])), b_own)
    sum_b = SumB(0)
    sum_b.begin(pack_dup(b_rows))
    sum_c = SumC(0)
    sum_c.begin(full_dot(jnp.transpose(c_pad[...]), chooser(c_base, nc, width, c_pad.shape[0]))[:RANK])

    sub = 64

    def split_rows(n, peak):
        rows = pl.ds(pl.multiple_of(n * sub, sub), sub)
        value = x_stage[rows, :]
        high, mid, low = split3(value)
        x_hi[rows, :] = high
        x_mid[rows, :] = mid
        x_low[rows, :] = low
        size = jnp.abs(value)
        for m in range(sub // 8):
            for q in range(width // LANES):
                peak = jnp.maximum(peak, size[m * 8:m * 8 + 8, q * LANES:(q + 1) * LANES])
        return peak

    def split_chunks(lo, hi, peak):
        for n in range(lo, hi):
            loads[n].wait()
            peak = lax.fori_loop(n * step // sub, (n + 1) * step // sub, split_rows, peak)
        return peak

    peak = split_chunks(0, 2, jnp.zeros((8, LANES), F32))
    sum_c.join()
    sum_b.join()
    peak = split_chunks(2, CHUNKS, peak)
    s_core[core] = peak
    s_copy = links.copy(s_core.at[core], s_core.at[core], partner)
    sum_c.turn()
    sum_b.turn()
    s_copy.wait_recv()
    s_buf[xx] = jnp.maximum(s_core[0], s_core[1])
    s_copies = spread(s_buf, "x")
    sum_c.share()
    b_pack = sum_b.finish()
    b_dup = unpack_dup(b_pack)
    peak = gather(s_buf, "x", s_copies, jnp.maximum)
    gram_sum_b = GramSum(0, "y")
    gram_sum_b.start(gram_of_packed(b_pack), peak)
    ct = sum_c.result()
    gram_b, peak = gram_sum_b.finish()
    gram_sum_c = GramSum(1, "z")
    gram_sum_c.start(gram_of_ct(ct), peak)

    inv_b_row = jnp.ones((1, LANES), F32)
    inv_b_col = jnp.ones((RANK, 1), F32)

    def inv_norms(gram):
        return 1.0 / jnp.sqrt(diag_row(gram)), 1.0 / jnp.sqrt(diag_col(gram))

    def system(gram_one, gram_two, row_scale, col_scale):
        row_wide = row_scale + swap_halves(row_scale)
        ridge = jnp.where(eye_mask(), lam_ref[0, 0], 0.0)
        mat = gram_one * gram_two * row_wide * col_scale + ridge
        unit = jnp.where(iota((RANK, LANES), 0) + RANK == iota((RANK, LANES), 1), 1.0, 0.0)
        inv_ref[...] = jnp.where(left_half((RANK, LANES)), mat, unit)

    def invert(lo, hi):
        inv_ref[...] = lax.fori_loop(lo, hi, lambda n, state: eliminate(state), inv_ref[...])

    def inverse():
        return jnp.where(left_half((RANK, LANES)), inv_ref[...], 0.0)

    def twice(mat):
        return jnp.concatenate([mat, swap_halves(mat)], axis=0)

    inv_c_row = inv_c_col = None
    inv_s = None
    for sweep in range(SWEEPS):
        wide = jnp.transpose(jnp.concatenate([ct, ct], axis=0))
        c_hi, c_mid, c_low = split3(wide)
        c_hi, c_mid, c_low = c_hi.astype(F32), c_mid.astype(F32), c_low.astype(F32)
        is_left = left_half(wide.shape)
        none = jnp.zeros_like(wide)
        w_hi = jnp.concatenate([jnp.where(is_left, c_hi, c_mid), jnp.where(is_left, c_low, none)], axis=1).astype(BF16)
        w_mid = jnp.concatenate([jnp.where(is_left, none, c_hi), jnp.where(is_left, c_mid, none)], axis=1).astype(BF16)
        w_low = jnp.concatenate([none, jnp.where(is_left, c_hi, none)], axis=1).astype(BF16)
        per = 16

        def t_step(n, unused, w_hi=w_hi, w_mid=w_mid, w_low=w_low, b_dup=b_dup):
            rows = pl.ds(pl.multiple_of(n * per * rows_j, per * rows_j), per * rows_j)
            prod = piece_dot(x_hi[rows, :], w_hi) + piece_dot(x_mid[rows, :], w_mid) + piece_dot(x_low[rows, :], w_low)
            t_val = prod[:, :LANES] + prod[:, LANES:]
            t_ref[rows, :] = t_val
            part = jnp.sum(t_val.reshape(per, rows_j, LANES) * b_dup[None], axis=1)
            pa_ref[pl.ds(pl.multiple_of(n * per, per), per), :] = part
            return unused

        lax.fori_loop(0, rows_i // per, t_step, 0)
        part = pa_ref[...]
        part = part + swap_halves(part)
        sum_a = SumA(sweep)
        sum_a.start(halves_of(pack_dup(part)))
        gram_c, top = gram_sum_c.finish()
        if sweep == 0:
            inv_c_row, inv_c_col = inv_b_row, inv_b_col
            inv_s = 1.0 / jnp.max(top, axis=(0, 1), keepdims=True)
            top_all = jnp.max(top, axis=(0, 1), keepdims=True)
            row_scale = jnp.where(left_half((1, LANES)), 1.0, 0.0)
            col_scale = jnp.ones((RANK, 1), F32)
        else:
            inv_c_row, inv_c_col = inv_norms(gram_c)
            row_scale, col_scale = inv_b_row * inv_c_row, inv_b_col * inv_c_col
        row_scale = jnp.where(left_half((1, LANES)), row_scale, 0.0)
        system(gram_b, gram_c, row_scale, col_scale)
        invert(0, 4)
        sum_a.turn()
        invert(4, 8)
        solver = twice(inverse() * (col_scale * inv_s))
        a_val = full_dot(sum_a.finish(), solver)
        a_pack[...] = a_val
        a_dup[...] = unpack_dup(a_val)
        gram_sum_a = GramSumA(2 + 3 * sweep, sweep)
        pad8 = jnp.zeros((8, LANES), F32)
        gram_sum_a.begin(gram_of_packed(a_val))
        def b_step(n, total):
            rows = pl.ds(pl.multiple_of(n * per * rows_j, per * rows_j), per * rows_j)
            t_val = t_ref[rows, :].reshape(per, rows_j, LANES)
            a_val = a_dup[pl.ds(pl.multiple_of(n * per, per), per), :]
            for m in range(per):
                total = total + t_val[m] * a_val[m:m + 1, :]
            return total

        part = lax.fori_loop(0, rows_i // per, b_step, jnp.zeros((rows_j, LANES), F32))
        part = part + swap_halves(part)
        sum_b = SumB(1 + sweep)
        sum_b.begin(pack_dup(part))
        gram_sum_a.join()
        sum_b.join()
        gram_a, unused_top = gram_sum_a.finish()
        inv_a_row, inv_a_col = inv_norms(gram_a)
        inv_a_row = jnp.where(left_half((1, LANES)), inv_a_row, 0.0)
        if sweep == 0:
            row_scale, col_scale = inv_a_row, inv_a_col
        else:
            row_scale, col_scale = inv_a_row * inv_c_row, inv_a_col * inv_c_col
        row_scale = jnp.where(left_half((1, LANES)), row_scale, 0.0)
        system(gram_a, gram_c, row_scale, col_scale)
        sum_b.turn()
        invert(0, 8)
        solver = twice(inverse() * (col_scale * inv_s))
        b_pack = full_dot(sum_b.finish(), solver)
        b_dup = unpack_dup(b_pack)
        gram_sum_b = GramSum(3 + 3 * sweep, "y")
        gram_sum_b.start(gram_of_packed(b_pack))
        acc_ref[...] = jnp.zeros_like(acc_ref)
        grp = 8

        def c_step(n, unused, b_dup=b_dup):
            a_val = a_pack[pl.ds(pl.multiple_of(n * grp, grp), grp), :]
            prod = jnp.concatenate([a_val[m:m + 1, :] * b_dup for m in range(grp)], axis=0)
            high, mid, low = split3(jnp.transpose(prod))
            for h in range(2):
                start = n * grp * rows_j + h * (rows_x // 2)
                rows = pl.ds(pl.multiple_of(start, grp * rows_j), grp * rows_j)
                side = slice(h * RANK, (h + 1) * RANK)
                left = jnp.concatenate([high[side], mid[side], low[side]], axis=0)
                acc_ref[...] += piece_dot(left, x_hi[rows, :])
                acc_ref[0:2 * RANK, :] += piece_dot(left[:2 * RANK], x_mid[rows, :])
                acc_ref[0:RANK, :] += piece_dot(left[:RANK], x_low[rows, :])
            return unused

        lax.fori_loop(0, rows_i // 2 // grp, c_step, 0)
        sum_c = SumC(1 + sweep)
        sum_c.begin(acc_ref[0:RANK, :] + acc_ref[RANK:2 * RANK, :] + acc_ref[2 * RANK:, :])
        gram_b, unused_top = gram_sum_b.finish()
        inv_b_row, inv_b_col = inv_norms(gram_b)
        row_scale, col_scale = inv_a_row * inv_b_row, inv_a_col * inv_b_col
        row_scale = jnp.where(left_half((1, LANES)), row_scale, 0.0)
        system(gram_a, gram_b, row_scale, col_scale)
        sum_c.join()
        invert(0, 4)
        sum_c.turn()
        invert(4, 8)
        sum_c.share()
        solver = inverse() * (row_scale * inv_s)
        ct = full_dot(solver[:, :RANK], sum_c.result())
        gram_sum_c = GramSum(4 + 3 * sweep, "z")
        gram_sum_c.start(gram_of_ct(ct))

    a_rows = full_dot(chooser(a_base, na, rows_i, c_pad.shape[0] if na <= c_pad.shape[0] else na), a_dup[...]) * inv_a_row
    a_out[...] = a_rows[:na, :RANK]
    b_rows = full_dot(chooser(b_base, nb, rows_j, b_pad.shape[0]), b_dup) * inv_b_row
    b_out[...] = b_rows[:nb, :RANK]
    c_rows = full_dot_nt(chooser(c_base, nc, width, c_pad.shape[0]), ct)
    gram_c, unused_top = gram_sum_c.finish()
    norm_c = jnp.sqrt(diag_row(gram_c))
    c_out[...] = c_rows[:nc, :] / norm_c[:, :RANK]
    w_out[...] = (norm_c * top_all)[:, :RANK]
    links.drain()


def b_buf_rows(b_core):
    return 2 * b_core.shape[2]


def solution(mesh):
    nx, ny, nz = mesh.shape["ix"] // 2, mesh.shape["jy"], mesh.shape["kz"]
    sizes = (nx, ny, nz)

    def body(x_blk, b_loc, c_loc, ridge):
        rows_i, rows_j, width = x_blk.shape
        rows_x = rows_i * rows_j
        nb, nc, na = b_loc.shape[0], c_loc.shape[0], rows_i // (ny * nz)
        big = max(nx, ny, nz)
        copies = count_copies(nx, ny, nz)
        vmem = pl.BlockSpec(memory_space=pltpu.VMEM)
        up8 = lambda n: -(-n // 8) * 8
        up16 = lambda n: -(-n // 16) * 16
        outs = pl.pallas_call(
            functools.partial(kernel, sizes),
            out_shape=(
                jax.ShapeDtypeStruct((na, RANK), F32),
                jax.ShapeDtypeStruct((nb, RANK), F32),
                jax.ShapeDtypeStruct((nc, RANK), F32),
                jax.ShapeDtypeStruct((1, RANK), F32),
            ),
            in_specs=[pl.BlockSpec(memory_space=pl.ANY), vmem, vmem, pl.BlockSpec(memory_space=pltpu.SMEM)],
            out_specs=(vmem, vmem, vmem, vmem),
            scratch_shapes=[
                pltpu.VMEM((rows_x, width), F32),
                pltpu.VMEM((rows_x, width), BF16),
                pltpu.VMEM((rows_x, width), BF16),
                pltpu.VMEM((rows_x, width), BF16),
                pltpu.VMEM((rows_x, LANES), F32),
                pltpu.VMEM((rows_i, LANES), F32),
                pltpu.VMEM((rows_i, LANES), F32),
                pltpu.VMEM((rows_i // 2, LANES), F32),
                pltpu.VMEM((3 * RANK, width), F32),
                pltpu.VMEM((up8(nb), LANES), F32),
                pltpu.VMEM((up16(nc), LANES), F32),
                pltpu.VMEM((RANK, LANES), F32),
                pltpu.VMEM((SWEEPS, 2, 2, big, rows_i // 4, LANES), F32),
                pltpu.VMEM((SWEEPS + 1, 2, rows_j // 2, LANES), F32),
                pltpu.VMEM((SWEEPS + 1, 2, 2, big, rows_j // 4, LANES), F32),
                pltpu.VMEM((SWEEPS + 1, RANK, width), F32),
                pltpu.VMEM((SWEEPS + 1, RANK // 2, width), F32),
                pltpu.VMEM((SWEEPS + 1, 2, 2, big, RANK // 4, width), F32),
                pltpu.VMEM((SWEEPS + 1, RANK, width), F32),
                pltpu.VMEM((SWEEPS, 2, 32, LANES), F32),
                pltpu.VMEM((2 + 3 * SWEEPS, big, GRAM_ROWS, LANES), F32),
                pltpu.VMEM((2, 8, LANES), F32),
                pltpu.VMEM((big, 8, LANES), F32),
                pltpu.SemaphoreType.DMA((CHUNKS,)),
                pltpu.SemaphoreType.DMA((copies,)),
                pltpu.SemaphoreType.DMA((copies,)),
            ],
            compiler_params=pltpu.CompilerParams(collective_id=0, has_side_effects=True, vmem_limit_bytes=60 * 1024 * 1024),
            name="cp_als",
        )(x_blk.reshape(rows_x, width), b_loc, c_loc, ridge.reshape(1, 1))
        a_loc, b_new, c_new, weights = outs
        return a_loc, b_new, c_new, weights.reshape(RANK)

    return jax.shard_map(
        body,
        mesh=mesh,
        in_specs=(P('ix', 'jy', 'kz'), P(('jy', 'ix', 'kz'), None), P(('kz', 'ix', 'jy'), None), P()),
        out_specs=(P(('ix', 'jy', 'kz'), None), P(('jy', 'ix', 'kz'), None), P(('kz', 'ix', 'jy'), None), P(None)),
        check_vma=False,
    )
```
